32 devices in a mesh: groups: 2 (over x), attn: 4 (over y, core), expert: 4 (over z).
Axes of the slice: x: 2, y: 2, z: 4, core: 2. Of those that a mesh axis runs over, the one named last changes fastest.
Arguments:
- tokens: bfloat16 [1024, 4096], P(('groups', 'attn'), 'expert'), parts along dimension 0, may hold values from -6 to 6
- expert_ids: int32 [1024, 8], P(('groups', 'attn')), parts along dimension 0, may hold values from 0 to 15, all different within a row; in each aligned block of 128 rows (0 to 127, 128 to 255, ...) at most 128 rows name the same one
- gate_weight: bfloat16 [1024, 8], P(('groups', 'attn')), parts along dimension 0, may hold values from 0.049804688 to 0.29882812
- w_gate: bfloat16 [16, 4096, 768], P('attn', 'expert'), may hold values from -0.09375 to 0.09375
- w_up: bfloat16 [16, 4096, 768], P('attn', 'expert'), may hold values from -0.09375 to 0.09375
- w_down: bfloat16 [16, 768, 4096], P('attn', None, 'expert'), may hold values from -0.21875 to 0.21875
- query: bfloat16 [64, 64, 128], P(('groups', 'attn', 'expert')), parts along dimension 0, may hold values from -100 to 100
- cache_k: bfloat16 [64, 768, 4, 128], P(('groups', 'attn', 'expert')), parts along dimension 0, may hold values from -6 to 6
- cache_v: bfloat16 [64, 768, 4, 128], P(('groups', 'attn', 'expert')), parts along dimension 0, may hold values from -6 to 6
- lengths: int32 [64], P(('groups', 'attn', 'expert')), parts along dimension 0, may hold values from 2 to 768, as said below
Outputs:
- moe_out: bfloat16 [1024, 4096], P(('groups', 'attn'), 'expert'), parts along dimension 0
- attn_out: bfloat16 [64, 8192], P(('groups', 'attn', 'expert')), parts along dimension 0
The draws below stay inside these ranges and needn't reach their ends.
There are 2 independent parts, one for each index of `groups`. The reference program is written for one: setup_inputs(seed, part) draws one part's arguments, and reference() takes and returns one part's arrays. A program takes and returns all parts, laid end to end along the dimension named above; an argument that names none is the same for every part. Nothing has to cross between parts.
Inputs may be any that keep to these rules, and one draw needn't show every extreme that they name: `expert_ids`: each row names 8 different experts. In the rows of one index of attn (aligned blocks of 128 rows) no expert is named by more than 128 rows, and in some block some expert by exactly 128. `lengths`: some sequence has all 768 positions live.
All inputs are finite; a program needn't handle non-finite values.
Results may differ from the reference program's by a relative error of at most 0.025.
Values may be sent and summed in bfloat16 or wider, within the bound.
A program may use at most 64 MiB of HBM per device.

```python
import math
import jax
import jax.numpy as jnp
import numpy as np
from jax import lax

D = 4096
FF = 768
TOPK = 8
TOK_DEV = 128
Q_HEADS = 64
KV_HEADS = 4
HEAD_DIM = 128
CTX = 768
EXPERTS = 16
TOKENS = 512
SEQS = 32
FEAT_DEV = 1024
CAPACITY = 256
SLOT = 128
N_EXPERT = 4


def attention_inputs(key):
    keys_key = jax.random.fold_in(key, 101)
    query_key = jax.random.fold_in(key, 102)
    shape_keys = (SEQS, CTX, KV_HEADS, HEAD_DIM)
    shape_query = (SEQS, Q_HEADS, HEAD_DIM)
    key_rows = jnp.clip(jax.random.normal(keys_key, shape_keys, jnp.float32), -6.0, 6.0)
    query_rows = jnp.clip(jax.random.normal(query_key, shape_query, jnp.float32), -6.0, 6.0)
    return (key_rows, query_rows)


def draw_query(key, part):
    return attention_inputs(key)[1].astype(jnp.bfloat16)


def draw_cache_k(key, part):
    return attention_inputs(key)[0].astype(jnp.bfloat16)


def draw_lengths(key, part):
    base_lengths = jax.random.randint(jax.random.fold_in(key, 201), (SEQS,), 2, CTX + 1, dtype=jnp.int32)
    full_index = jax.random.randint(jax.random.fold_in(key, 202), (), 0, SEQS, dtype=jnp.int32)
    return jnp.where(jnp.arange(SEQS, dtype=jnp.int32) == full_index, CTX, base_lengths).astype(jnp.int32)


def block_scale(own_key, shape, cuts, smallest, top_value):
    factor_of = 1.0
    for axis_at, shards_of in cuts:
        steps = jax.random.uniform(jax.random.fold_in(jax.random.fold_in(own_key, 6), axis_at), (shards_of,), jnp.float32, smallest / len(cuts), top_value / len(cuts))
        factor_of = factor_of * jnp.repeat(jnp.exp(steps), shape[axis_at] // shards_of).reshape((-1,) + (1,) * (len(shape) - 1 - axis_at))
    return factor_of


def deal_out(stream_key, own, number, rows, count, top, most, slope):
    order = jax.random.permutation(stream_key, count)
    crowded, ordinary = shares(count, rows * top, most, slope, True), shares(count, rows * top, most, slope, False)
    places = jnp.arange(count)

    def named(sizes, offset_by):
        used = int((sizes > 0).sum())
        fixed = max(1, used // 4)
        passed = fixed + (places - fixed + offset_by * (used - fixed)) % max(1, count - fixed)
        return jnp.zeros((count,), jnp.int32).at[order[jnp.where(places < fixed, places, passed)]].set(jnp.asarray(sizes, jnp.int32))

    sizes = jnp.where(number % 4 == 0, named(crowded, number // 4), named(ordinary, number - number // 4 - 1))
    mixed = jax.random.permutation(jax.random.fold_in(own, 3), count)
    donor, taker = mixed[0:count // 2 * 2:2], mixed[1:count // 2 * 2:2]
    margin = jnp.minimum(sizes[donor] - 1, most - sizes[taker]) // 2
    margin = jnp.where((donor == order[0]) | (taker == order[0]) | (sizes[taker] == 0), 0, jnp.maximum(margin, 0))
    passed = jax.random.randint(jax.random.fold_in(own, 4), (count // 2,), 0, 1 << 20) % (margin + 1)
    sizes = sizes.at[donor].add(-passed).at[taker].add(passed)
    items = jnp.searchsorted(jnp.cumsum(sizes), jnp.arange(rows * top), side="right").astype(jnp.int32)
    table = items.reshape(top, rows).T
    table = table[jax.random.permutation(jax.random.fold_in(own, 1), rows)]
    offset_by = jax.random.randint(jax.random.fold_in(own, 2), (rows, 1), 0, top)
    return jnp.take_along_axis(table, (jnp.arange(top)[None, :] + offset_by) % top, axis=1)


def shares(number_of, total, reach, slope, full):
    portions = [(1 << 20) // math.isqrt(rank ** slope) + 1 for rank in range(1, number_of + 1)]
    largest = reach if full else min(reach, max(-(-total // number_of), total * portions[0] // sum(portions)))
    least = 1 if total - largest >= number_of - 1 else 0
    given, rest = [largest] + [least] * (number_of - 1), total - largest - least * (number_of - 1)
    while rest > 0:
        movable = [i for i in range(1, number_of) if given[i] < largest] or [i for i in range(1, number_of) if given[i] < reach]
        mass, remaining = sum([portions[i] for i in movable]), rest
        for i in movable:
            addition = min(reach - given[i], max(1, remaining * portions[i] // mass), rest)
            given[i] = given[i] + addition
            rest = rest - addition
    return np.array(given)


def centred(rng, extent, scale, reach, split=(), held_as=jnp.bfloat16):
    values = scale * jax.random.normal(rng, extent, jnp.float32)
    if split:
        values = values * block_scale(rng, extent, split, -0.22, 0.18)
    return jnp.clip(values, -reach, reach).astype(held_as)


def setup_inputs(seed: int = 0, part: int = 0) -> dict:
    keys = jax.random.split(jax.random.key(seed), 11)
    own_keys = jax.random.split(jax.random.fold_in(keys[10], part), 11)
    tokens = centred(own_keys[0], (TOKENS, D), 1.0, 6.0, ((0, 4), (1, 4)))
    expert_ids_keys = jax.random.split(jax.random.fold_in(own_keys[1], 1), TOKENS // TOK_DEV)
    expert_ids_turns = jax.random.permutation(jax.random.fold_in(own_keys[1], 3), TOKENS // TOK_DEV)
    expert_ids = jax.vmap(lambda own, number: deal_out(jax.random.fold_in(own_keys[1], 2), own, number, TOK_DEV, EXPERTS, TOPK, SLOT, 2))(expert_ids_keys, expert_ids_turns).reshape((TOKENS, TOPK))
    gate_weight = jnp.clip(0.049804688 + 0.24902344 * jax.random.uniform(own_keys[2], (TOKENS, TOPK), jnp.float32) ** block_scale(own_keys[2], (TOKENS, TOPK), ((0, 4),), -0.2, 0.2), 0.049804688, 0.29882812).astype(jnp.bfloat16)
    w_gate = centred(keys[3], (EXPERTS, D, FF), D ** -0.5, 0.09375, ((0, 4), (1, 4)))
    w_up = centred(keys[4], (EXPERTS, D, FF), D ** -0.5, 0.09375, ((0, 4), (1, 4)))
    w_down = centred(keys[5], (EXPERTS, FF, D), FF ** -0.5, 0.21875, ((0, 4), (2, 4)))
    query = draw_query(jax.random.fold_in(jax.random.fold_in(keys[10], part), 71), part)
    cache_k = draw_cache_k(jax.random.fold_in(jax.random.fold_in(keys[10], part), 71), part)
    cache_v = centred(own_keys[8], (SEQS, CTX, KV_HEADS, HEAD_DIM), 1.0, 6.0, ((0, 16),))
    lengths = draw_lengths(jax.random.fold_in(jax.random.fold_in(keys[10], part), 71), part)
    return {"tokens": tokens, "expert_ids": expert_ids, "gate_weight": gate_weight, "w_gate": w_gate, "w_up": w_up, "w_down": w_down, "query": query, "cache_k": cache_k, "cache_v": cache_v, "lengths": lengths}


def one_expert(operands):
    expert_rows, gate_mat, up_mat, down_mat = operands
    blocked = expert_rows.astype(jnp.float32).reshape(CAPACITY, N_EXPERT, FEAT_DEV)
    both_mats = jnp.concatenate([gate_mat, up_mat], axis=1).astype(jnp.float32).reshape(N_EXPERT, FEAT_DEV, 2 * FF)
    partials = jnp.einsum("rbd,bdf->brf", blocked, both_mats)
    rounded = lax.optimization_barrier(partials.astype(jnp.bfloat16))
    both_sums = jnp.sum(rounded.astype(jnp.float32), axis=0)
    hidden = (jax.nn.silu(both_sums[:, :FF]) * both_sums[:, FF:]).astype(jnp.bfloat16)
    return jnp.dot(hidden, down_mat, preferred_element_type=jnp.float32).astype(jnp.bfloat16)


def reference(tokens, expert_ids, gate_weight, w_gate, w_up, w_down, query, cache_k, cache_v, lengths):
    total_rows = tokens.shape[0]
    experts = w_gate.shape[0]
    wanted = jnp.arange(experts, dtype=jnp.int32)
    member = jnp.any(expert_ids[:, :, None] == wanted[None, None, :], axis=1).astype(jnp.int32)
    position = jnp.cumsum(member, axis=0, dtype=jnp.int32) - member
    taken = (member > 0) & (position < CAPACITY)
    target = jnp.where(taken, wanted[None, :] * CAPACITY + position, experts * CAPACITY)
    owners = jnp.broadcast_to(jnp.arange(total_rows, dtype=jnp.int32)[:, None], (total_rows, experts))
    token_index = jnp.full((experts * CAPACITY,), total_rows, jnp.int32).at[target.reshape(-1)].set(owners.reshape(-1), mode="drop")
    padded = jnp.concatenate([tokens, jnp.zeros((1, D), tokens.dtype)], axis=0)
    packed = padded[token_index].reshape(experts, CAPACITY, D)
    results = lax.map(one_expert, (packed, w_gate, w_up, w_down))
    results = lax.optimization_barrier(results)
    place_of = jnp.take_along_axis(position, expert_ids, axis=1)
    keep_mask = place_of < CAPACITY
    flat_index = jnp.where(keep_mask, expert_ids * CAPACITY + place_of, 0)
    picked = results.reshape(experts * CAPACITY, D)[flat_index]
    factor = jnp.where(keep_mask, gate_weight.astype(jnp.float32), 0.0)
    moe_out = jnp.sum(factor[:, :, None] * picked.astype(jnp.float32), axis=1).astype(jnp.bfloat16)

    seq_count = query.shape[0]
    grouped = query.astype(jnp.float32).reshape(seq_count, KV_HEADS, Q_HEADS // KV_HEADS, HEAD_DIM)
    scores = jnp.einsum("skgd,slkd->skgl", grouped, cache_k.astype(jnp.float32)) * (HEAD_DIM ** -0.5)
    live_mask = jnp.arange(CTX, dtype=jnp.int32)[None, None, None, :] < lengths[:, None, None, None]
    masked = jnp.where(live_mask, scores, -jnp.inf)
    row_peak = jnp.max(masked, axis=3, keepdims=True)
    weighted = jnp.exp(masked - row_peak)
    denominator = jnp.sum(weighted, axis=3, keepdims=True)
    prob_bf = lax.optimization_barrier((weighted / denominator).astype(jnp.bfloat16))
    attended = jnp.einsum("skgl,slkd->skgd", prob_bf.astype(jnp.float32), cache_v.astype(jnp.float32))
    attn_out = attended.reshape(seq_count, Q_HEADS * HEAD_DIM).astype(jnp.bfloat16)
    return (moe_out, attn_out)
```

```python
import functools

import jax
import jax.numpy as jnp
from jax import lax
from jax.experimental import pallas as pl
from jax.experimental.pallas import tpu as pltpu
from jax.sharding import PartitionSpec as P

F32 = jnp.float32
BF16 = jnp.bfloat16


def remote(src, dst, send_sem, recv_sem, axis, peer):
    return pltpu.make_async_remote_copy(
        src_ref=src,
        dst_ref=dst,
        send_sem=send_sem,
        recv_sem=recv_sem,
        device_id={axis: peer},
        device_id_type=pl.DeviceIdType.MESH,
    )


def moe_kernel(
    n_attn,
    n_exp,
    experts,
    tok_ref,
    meta_ref,
    wg_hbm,
    wu_hbm,
    wd_hbm,
    out_ref,
    wg,
    wu,
    wd,
    tok_all,
    meta_all,
    pos_col,
    pos_row,
    part,
    part_in,
    hid,
    acc,
    ret,
    ret_in,
    w_sem,
    tok_s,
    tok_r,
    meta_s,
    meta_r,
    part_s,
    part_r,
    hid_s,
    hid_r,
    ret_s,
    ret_r,
):
    me = lax.axis_index("attn")
    mine = lax.axis_index("expert")
    local = wg.shape[0]
    rows = tok_ref.shape[0]
    feat = tok_ref.shape[1]
    width = meta_ref.shape[1]
    ffn = wg.shape[2]
    slots = part.shape[2]
    capacity = n_exp * slots
    all_rows = n_attn * rows

    def weight_copy(i, j):
        src, dst = ((wg_hbm, wg), (wu_hbm, wu), (wd_hbm, wd))[i]
        return pltpu.make_async_copy(src.at[j], dst.at[j], w_sem.at[i, j])

    for j in range(local):
        weight_copy(0, j).start()
        weight_copy(1, j).start()
    for j in range(local):
        weight_copy(2, j).start()

    barrier = pltpu.get_barrier_semaphore()
    for d in range(1, n_attn):
        pl.semaphore_signal(
            barrier, inc=1, device_id={"attn": lax.rem(me + d, n_attn)},
            device_id_type=pl.DeviceIdType.MESH,
        )
    for d in range(1, n_exp):
        pl.semaphore_signal(
            barrier, inc=1, device_id={"expert": lax.rem(mine + d, n_exp)},
            device_id_type=pl.DeviceIdType.MESH,
        )
    pl.semaphore_wait(barrier, n_attn + n_exp - 2)

    def meta_copy(d, slot):
        return remote(meta_ref, meta_all.at[slot], meta_s.at[d - 1], meta_r.at[d - 1],
                      "attn", lax.rem(me + d, n_attn))

    def tok_copy(d, slot):
        return remote(tok_ref, tok_all.at[slot], tok_s.at[d - 1], tok_r.at[d - 1],
                      "attn", lax.rem(me + d, n_attn))

    for d in range(1, n_attn):
        meta_copy(d, me).start()
    for d in range(1, n_attn):
        tok_copy(d, me).start()
    tok_all[me] = tok_ref[...]
    meta_all[me] = meta_ref[...]
    for d in range(1, n_attn):
        meta_copy(d, lax.rem(me + n_attn - d, n_attn)).wait_recv()

    below = (
        lax.broadcasted_iota(jnp.int32, (rows, rows), 0)
        > lax.broadcasted_iota(jnp.int32, (rows, rows), 1)
    ).astype(F32).astype(BF16)
    offset = jnp.zeros((1, width), F32)
    for b in range(n_attn):
        block = meta_all[b]
        place = jnp.dot(below, block, preferred_element_type=F32) + offset
        wide = block.astype(F32)
        offset = offset + jnp.sum(wide, axis=0, keepdims=True)
        place = jnp.where(wide > 0.5, place, -1.0)
        pos_col[b] = place
        pos_row[:, b * rows:(b + 1) * rows] = place.T

    for d in range(1, n_attn):
        tok_copy(d, lax.rem(me + n_attn - d, n_attn)).wait_recv()

    def part_copy(j, d):
        peer = lax.rem(mine + d, n_exp)
        return remote(part.at[j, peer], part_in.at[j, d - 1], part_s.at[j, d - 1],
                      part_r.at[j, d - 1], "expert", peer)

    def hid_copy(j, d, slot):
        return remote(hid.at[j, mine], hid.at[j, slot], hid_s.at[j, d - 1],
                      hid_r.at[j, d - 1], "expert", lax.rem(mine + d, n_exp))

    def first(j, carry):
        place = pos_row[pl.ds(me * local + j, 1), :].astype(jnp.int32)
        chosen = lax.broadcasted_iota(jnp.int32, (capacity, all_rows), 0) == place
        packed = jnp.dot(
            chosen.astype(F32).astype(BF16),
            tok_all[...].reshape(all_rows, feat),
            preferred_element_type=F32,
        ).astype(BF16)
        weight_copy(0, j).wait()
        weight_copy(1, j).wait()
        gate = jnp.dot(packed, wg[j], preferred_element_type=F32).astype(BF16)
        part[j, :, :, :ffn] = gate.reshape(n_exp, slots, ffn)
        up = jnp.dot(packed, wu[j], preferred_element_type=F32).astype(BF16)
        part[j, :, :, ffn:] = up.reshape(n_exp, slots, ffn)
        for d in range(1, n_exp):
            part_copy(j, d).start()
        return carry

    lax.fori_loop(0, local, first, 0)

    def second(j, carry):
        for d in range(1, n_exp):
            part_copy(j, d).wait_recv()
        both = part[j, mine].astype(F32)
        for d in range(1, n_exp):
            both = both + part_in[j, d - 1].astype(F32)
        gate = both[:, :ffn]
        hid[j, mine] = (gate / (1.0 + jnp.exp(-gate)) * both[:, ffn:]).astype(BF16)
        for d in range(1, n_exp):
            hid_copy(j, d, mine).start()
        return carry

    lax.fori_loop(0, local, second, 0)

    acc[...] = jnp.zeros_like(acc)

    def third(j, carry):
        for d in range(1, n_exp):
            hid_copy(j, d, lax.rem(mine + n_exp - d, n_exp)).wait_recv()
        weight_copy(2, j).wait()
        result = jnp.dot(
            hid[j].reshape(capacity, ffn), wd[j], preferred_element_type=F32
        ).astype(BF16)
        column = me * local + j
        lanes = lax.broadcasted_iota(jnp.int32, (rows, width), 1)
        slot_ids = lax.broadcasted_iota(jnp.int32, (rows, capacity), 1)

        def combine(b, inner):
            place = jnp.sum(
                jnp.where(lanes == column, pos_col[b], 0.0), axis=1, keepdims=True
            ).astype(jnp.int32)
            factor = jnp.sum(
                jnp.where(lanes == column + experts, meta_all[b].astype(F32), 0.0),
                axis=1, keepdims=True,
            )
            spread = jnp.where(slot_ids == place, factor, 0.0).astype(BF16)
            acc[b] = acc[b] + jnp.dot(spread, result, preferred_element_type=F32)
            return inner

        for b in range(n_attn):
            combine(b, 0)
        return carry

    lax.fori_loop(0, local, third, 0)

    ret[...] = acc[...].astype(BF16)

    def ret_copy(d):
        peer = lax.rem(me + d, n_attn)
        return remote(ret.at[peer], ret_in.at[d - 1], ret_s.at[d - 1], ret_r.at[d - 1],
                      "attn", peer)

    for d in range(1, n_attn):
        ret_copy(d).start()
    total = acc[me]
    for d in range(1, n_attn):
        ret_copy(d).wait_recv()
        total = total + ret_in[d - 1].astype(F32)
    out_ref[...] = total.astype(BF16)

    for d in range(1, n_attn):
        meta_copy(d, me).wait_send()
        tok_copy(d, me).wait_send()
        ret_copy(d).wait_send()

    def drain(j, carry):
        for d in range(1, n_exp):
            part_copy(j, d).wait_send()
            hid_copy(j, d, mine).wait_send()
        return carry

    lax.fori_loop(0, local, drain, 0)


def routed(tokens, expert_ids, gate_weight, w_gate, w_up, w_down, n_attn, n_exp):
    rows, feat = tokens.shape
    local, _, ffn = w_gate.shape
    feat_out = w_down.shape[2]
    experts = local * n_attn
    capacity = rows * expert_ids.shape[1] // local
    slots = capacity // n_exp
    width = -(-2 * experts // 128) * 128
    wanted = jnp.arange(width, dtype=jnp.int32)[None, None, :]
    ids = expert_ids[:, :, None]
    gates = gate_weight.astype(F32)[:, :, None]
    meta = jnp.sum(
        jnp.where(ids == wanted, 1.0, jnp.where(ids + experts == wanted, gates, 0.0)),
        axis=1,
    ).astype(BF16)
    dma = pltpu.SemaphoreType.DMA
    vmem = pltpu.VMEM
    return pl.pallas_call(
        functools.partial(moe_kernel, n_attn, n_exp, experts),
        out_shape=jax.ShapeDtypeStruct((rows, feat_out), BF16),
        in_specs=[pl.BlockSpec(memory_space=pltpu.VMEM)] * 2
        + [pl.BlockSpec(memory_space=pl.ANY)] * 3,
        out_specs=pl.BlockSpec(memory_space=pltpu.VMEM),
        scratch_shapes=[
            vmem(w_gate.shape, BF16),
            vmem(w_up.shape, BF16),
            vmem(w_down.shape, BF16),
            vmem((n_attn, rows, feat), BF16),
            vmem((n_attn, rows, width), BF16),
            vmem((n_attn, rows, width), F32),
            vmem((width, n_attn * rows), F32),
            vmem((local, n_exp, slots, 2 * ffn), BF16),
            vmem((local, n_exp - 1, slots, 2 * ffn), BF16),
            vmem((local, n_exp, slots, ffn), BF16),
            vmem((n_attn, rows, feat_out), F32),
            vmem((n_attn, rows, feat_out), BF16),
            vmem((n_attn - 1, rows, feat_out), BF16),
            dma((3, local)),
            dma((n_attn - 1,)),
            dma((n_attn - 1,)),
            dma((n_attn - 1,)),
            dma((n_attn - 1,)),
            dma((local, n_exp - 1)),
            dma((local, n_exp - 1)),
            dma((local, n_exp - 1)),
            dma((local, n_exp - 1)),
            dma((n_attn - 1,)),
            dma((n_attn - 1,)),
        ],
        compiler_params=pltpu.CompilerParams(
            collective_id=0, has_side_effects=True, vmem_limit_bytes=52 * 1024 * 1024
        ),
    )(tokens, meta, w_gate, w_up, w_down)


def grouped_attention(query, cache_k, cache_v, lengths):
    seq_count, head_total, head_size = query.shape
    context = cache_k.shape[1]
    kv_count = cache_k.shape[2]
    grouped = query.reshape(seq_count, kv_count, head_total // kv_count, head_size)
    scores = jnp.einsum(
        "skgd,slkd->skgl", grouped, cache_k, preferred_element_type=jnp.float32
    ) * head_size ** (-0.5)
    live_mask = (
        lax.broadcasted_iota(jnp.int32, (seq_count, 1, 1, context), 3)
        < lengths[:, None, None, None]
    )
    masked = jnp.where(live_mask, scores, -jnp.inf)
    row_peak = jnp.max(masked, axis=3, keepdims=True)
    weighted = jnp.exp(masked - row_peak)
    denominator = jnp.sum(weighted, axis=3, keepdims=True)
    prob_bf = (weighted / denominator).astype(jnp.bfloat16)
    attended = jnp.einsum("skgl,slkd->skgd", prob_bf, cache_v, preferred_element_type=jnp.float32)
    return attended.reshape(seq_count, head_total * head_size).astype(jnp.bfloat16)


def body(tokens, expert_ids, gate_weight, w_gate, w_up, w_down, query, cache_k, cache_v, lengths):
    n_attn = lax.axis_size("attn")
    n_exp = lax.axis_size("expert")
    moe_out = routed(
        tokens, expert_ids, gate_weight, w_gate, w_up, w_down, n_attn, n_exp
    )
    attn_out = grouped_attention(query, cache_k, cache_v, lengths)
    return (moe_out, attn_out)


def solution(mesh):
    return jax.shard_map(
        body,
        mesh=mesh,
        in_specs=(
            P(("groups", "attn"), "expert"),
            P(("groups", "attn"), None),
            P(("groups", "attn"), None),
            P("attn", "expert", None),
            P("attn", "expert", None),
            P("attn", None, "expert"),
            P(("groups", "attn", "expert"), None, None),
            P(("groups", "attn", "expert"), None, None, None),
            P(("groups", "attn", "expert"), None, None, None),
            P(("groups", "attn", "expert")),
        ),
        out_specs=(P(("groups", "attn"), "expert"), P(("groups", "attn", "expert"), None)),
        check_vma=False,
    )
```

```python
import functools

import jax
import jax.numpy as jnp
from jax import lax
from jax.experimental import pallas as pl
from jax.experimental.pallas import tpu as pltpu
from jax.sharding import PartitionSpec as P

F32 = jnp.float32
BF16 = jnp.bfloat16


def remote(src, dst, send_sem, recv_sem, axis, peer):
    return pltpu.make_async_remote_copy(
        src_ref=src,
        dst_ref=dst,
        send_sem=send_sem,
        recv_sem=recv_sem,
        device_id={axis: peer},
        device_id_type=pl.DeviceIdType.MESH,
    )


def attend(length_ref, query_ref, ck_ref, cv_ref, att_ref, kv_count):
    seqs, heads, size = query_ref.shape
    span = ck_ref.shape[1]
    column = lax.broadcasted_iota(jnp.int32, (heads, span), 1)
    row = lax.broadcasted_iota(jnp.int32, (heads, span), 0)
    own = lax.rem(column, kv_count) == row // (heads // kv_count)
    for s in range(seqs):
        scores = lax.dot_general(
            query_ref[s], ck_ref[s], (((1,), (1,)), ((), ())),
            preferred_element_type=F32,
        ) * size ** (-0.5)
        live = own & (column < length_ref[s] * kv_count)
        masked = jnp.where(live, scores, -jnp.inf)
        peak = jnp.max(masked, axis=1, keepdims=True)
        weighted = jnp.exp(masked - peak)
        prob = (weighted / jnp.sum(weighted, axis=1, keepdims=True)).astype(BF16)
        att_ref[s] = jnp.dot(prob, cv_ref[s], preferred_element_type=F32).astype(BF16)


def moe_kernel(
    n_attn,
    n_exp,
    experts,
    kv_count,
    tok_ref,
    meta_ref,
    wg_hbm,
    wu_hbm,
    wd_hbm,
    length_ref,
    query_ref,
    ck_hbm,
    cv_hbm,
    out_ref,
    att_ref,
    wg,
    wu,
    wd,
    ck,
    cv,
    tok_all,
    meta_all,
    pos_col,
    pos_row,
    part,
    pair_in,
    part_in,
    hid,
    acc,
    ret,
    ret_in,
    w_sem,
    c_sem,
    tok_s,
    tok_r,
    meta_s,
    meta_r,
    pair_s,
    pair_r,
    part_s,
    part_r,
    hid_s,
    hid_r,
    back_s,
    back_r,
    ret_s,
    ret_r,
):
    me = lax.axis_index("attn")
    mine = lax.axis_index("expert")
    local = wg.shape[0]
    rows = tok_ref.shape[0]
    feat = tok_ref.shape[1]
    width = meta_ref.shape[1]
    ffn = wg.shape[2]
    pairs, half, slots = part.shape[1:4]
    side = lax.rem(mine, pairs)
    place_in_half = mine // pairs
    capacity = n_exp * slots
    all_rows = n_attn * rows

    def weight_copy(i, j):
        src, dst = ((wg_hbm, wg), (wu_hbm, wu), (wd_hbm, wd))[i]
        return pltpu.make_async_copy(src.at[j], dst.at[j], w_sem.at[i, j])

    for j in range(local):
        weight_copy(0, j).start()
        weight_copy(1, j).start()
    for j in range(local):
        weight_copy(2, j).start()

    ck_copy = pltpu.make_async_copy(ck_hbm, ck, c_sem.at[0])
    cv_copy = pltpu.make_async_copy(cv_hbm, cv, c_sem.at[1])
    ck_copy.start()
    cv_copy.start()

    barrier = pltpu.get_barrier_semaphore()
    for d in range(1, n_attn):
        pl.semaphore_signal(
            barrier, inc=1, device_id={"attn": lax.rem(me + d, n_attn)},
            device_id_type=pl.DeviceIdType.MESH,
        )
    for d in range(1, n_exp):
        pl.semaphore_signal(
            barrier, inc=1, device_id={"expert": lax.rem(mine + d, n_exp)},
            device_id_type=pl.DeviceIdType.MESH,
        )
    pl.semaphore_wait(barrier, n_attn + n_exp - 2)

    def meta_copy(d, slot):
        return remote(meta_ref, meta_all.at[slot], meta_s.at[d - 1], meta_r.at[d - 1],
                      "attn", lax.rem(me + d, n_attn))

    def tok_copy(d, slot):
        return remote(tok_ref, tok_all.at[slot], tok_s.at[d - 1], tok_r.at[d - 1],
                      "attn", lax.rem(me + d, n_attn))

    for d in range(1, n_attn):
        meta_copy(d, me).start()
    for d in range(1, n_attn):
        tok_copy(d, me).start()
    tok_all[me] = tok_ref[...]
    meta_all[me] = meta_ref[...]
    for d in range(1, n_attn):
        meta_copy(d, lax.rem(me + n_attn - d, n_attn)).wait_recv()

    below = (
        lax.broadcasted_iota(jnp.int32, (rows, rows), 0)
        > lax.broadcasted_iota(jnp.int32, (rows, rows), 1)
    ).astype(F32).astype(BF16)
    offset = jnp.zeros((1, width), F32)
    for b in range(n_attn):
        block = meta_all[b]
        place = jnp.dot(below, block, preferred_element_type=F32) + offset
        wide = block.astype(F32)
        offset = offset + jnp.sum(wide, axis=0, keepdims=True)
        place = jnp.where(wide > 0.5, place, -1.0)
        pos_col[b] = place
        pos_row[:, b * rows:(b + 1) * rows] = place.T

    for d in range(1, n_attn):
        tok_copy(d, lax.rem(me + n_attn - d, n_attn)).wait_recv()

    def pair_copy(j):
        return remote(part.at[j, 1 - side], pair_in.at[j], pair_s.at[j], pair_r.at[j],
                      "expert", mine + 1 - 2 * side)

    def part_copy(j, d):
        other = lax.rem(place_in_half + d, half)
        return remote(part.at[j, side, other], part_in.at[j, d - 1], part_s.at[j, d - 1],
                      part_r.at[j, d - 1], "expert", other * pairs + side)

    def hid_copy(j, d, slot):
        other = lax.rem(place_in_half + d, half)
        return remote(hid.at[j, side, place_in_half], hid.at[j, side, slot],
                      hid_s.at[j, d - 1], hid_r.at[j, d - 1], "expert",
                      other * pairs + side)

    def hid_arrive(j):
        for d in range(1, half):
            hid_copy(j, d, lax.rem(place_in_half + half - d, half)).wait_recv()

    def back_copy(j, which):
        return remote(hid.at[j, side], hid.at[j, which], back_s.at[j], back_r.at[j],
                      "expert", mine + 1 - 2 * side)

    def first(j):
        place = pos_row[pl.ds(me * local + j, 1), :].astype(jnp.int32)
        chosen = lax.broadcasted_iota(jnp.int32, (capacity, all_rows), 0) == place
        packed = jnp.dot(
            chosen.astype(F32).astype(BF16),
            tok_all[...].reshape(all_rows, feat),
            preferred_element_type=F32,
        ).astype(BF16)
        weight_copy(0, j).wait()
        weight_copy(1, j).wait()
        gate = jnp.dot(packed, wg[j], preferred_element_type=F32).astype(BF16)
        part[j, :, :, :, :ffn] = gate.reshape(pairs, half, slots, ffn)
        up = jnp.dot(packed, wu[j], preferred_element_type=F32).astype(BF16)
        part[j, :, :, :, ffn:] = up.reshape(pairs, half, slots, ffn)
        if pairs > 1:
            pair_copy(j).start()

    def reduce_pair(j):
        if pairs > 1:
            pair_copy(j).wait_recv()
            part[j, side] = (part[j, side].astype(F32) + pair_in[j].astype(F32)).astype(BF16)
        for d in range(1, half):
            part_copy(j, d).start()

    def second(j):
        for d in range(1, half):
            part_copy(j, d).wait_recv()
        both = part[j, side, place_in_half].astype(F32)
        for d in range(1, half):
            both = both + part_in[j, d - 1].astype(F32)
        gate = both[:, :ffn]
        hid[j, side, place_in_half] = (
            gate / (1.0 + jnp.exp(-gate)) * both[:, ffn:]
        ).astype(BF16)
        for d in range(1, half):
            hid_copy(j, d, place_in_half).start()

    def pass_on(j):
        hid_arrive(j)
        if pairs > 1:
            back_copy(j, side).start()

    acc[...] = jnp.zeros_like(acc)

    def third(j):
        if pairs > 1:
            back_copy(j, 1 - side).wait_recv()
        weight_copy(2, j).wait()
        result = jnp.dot(
            hid[j].reshape(capacity, ffn), wd[j], preferred_element_type=F32
        ).astype(BF16)
        column = me * local + j
        lanes = lax.broadcasted_iota(jnp.int32, (rows, width), 1)
        slot_ids = lax.broadcasted_iota(jnp.int32, (rows, capacity), 1)

        def combine(b, inner):
            place = jnp.sum(
                jnp.where(lanes == column, pos_col[b], 0.0), axis=1, keepdims=True
            ).astype(jnp.int32)
            factor = jnp.sum(
                jnp.where(lanes == column + experts, meta_all[b].astype(F32), 0.0),
                axis=1, keepdims=True,
            )
            spread = jnp.where(slot_ids == place, factor, 0.0).astype(BF16)
            acc[b] = acc[b] + jnp.dot(spread, result, preferred_element_type=F32)
            return inner

        for b in range(n_attn):
            combine(b, 0)

    def step(s, carry):
        for lag, stage in enumerate((first, reduce_pair, second, pass_on, third)):
            if lag == 2:
                @pl.when(s == 1)
                def _():
                    attend(length_ref, query_ref, ck, cv, att_ref, kv_count)

            @pl.when((s >= lag) & (s < local + lag))
            def _():
                stage(s - lag)
        return carry

    ck_copy.wait()
    cv_copy.wait()
    lax.fori_loop(0, local + 4, step, 0)

    ret[...] = acc[...].astype(BF16)

    def ret_copy(d):
        peer = lax.rem(me + d, n_attn)
        return remote(ret.at[peer], ret_in.at[d - 1], ret_s.at[d - 1], ret_r.at[d - 1],
                      "attn", peer)

    for d in range(1, n_attn):
        ret_copy(d).start()
    total = acc[me]
    for d in range(1, n_attn):
        ret_copy(d).wait_recv()
        total = total + ret_in[d - 1].astype(F32)
    out_ref[...] = total.astype(BF16)

    for d in range(1, n_attn):
        meta_copy(d, me).wait_send()
        tok_copy(d, me).wait_send()
        ret_copy(d).wait_send()

    def drain(j, carry):
        if pairs > 1:
            pair_copy(j).wait_send()
            back_copy(j, side).wait_send()
        for d in range(1, half):
            part_copy(j, d).wait_send()
            hid_copy(j, d, place_in_half).wait_send()
        return carry

    lax.fori_loop(0, local, drain, 0)


def routed(tokens, expert_ids, gate_weight, w_gate, w_up, w_down, query, cache_k, cache_v, lengths, n_attn, n_exp):
    rows, feat = tokens.shape
    local, _, ffn = w_gate.shape
    feat_out = w_down.shape[2]
    experts = local * n_attn
    capacity = rows * expert_ids.shape[1] // local
    slots = capacity // n_exp
    pairs = 2 if n_exp > 2 and n_exp % 2 == 0 else 1
    half = n_exp // pairs
    width = -(-2 * experts // 128) * 128
    wanted = jnp.arange(width, dtype=jnp.int32)[None, None, :]
    ids = expert_ids[:, :, None]
    gates = gate_weight.astype(F32)[:, :, None]
    meta = jnp.sum(
        jnp.where(ids == wanted, 1.0, jnp.where(ids + experts == wanted, gates, 0.0)),
        axis=1,
    ).astype(BF16)
    seqs, heads, size = query.shape
    context, kv_count = cache_k.shape[1:3]
    flat = (seqs, context * kv_count, size)
    dma = pltpu.SemaphoreType.DMA
    vmem = pltpu.VMEM
    return pl.pallas_call(
        functools.partial(moe_kernel, n_attn, n_exp, experts, kv_count),
        out_shape=(
            jax.ShapeDtypeStruct((rows, feat_out), BF16),
            jax.ShapeDtypeStruct(query.shape, BF16),
        ),
        in_specs=[pl.BlockSpec(memory_space=pltpu.VMEM)] * 2
        + [pl.BlockSpec(memory_space=pl.ANY)] * 3
        + [pl.BlockSpec(memory_space=pltpu.SMEM)]
        + [pl.BlockSpec(memory_space=pltpu.VMEM)]
        + [pl.BlockSpec(memory_space=pl.ANY)] * 2,
        out_specs=[pl.BlockSpec(memory_space=pltpu.VMEM)] * 2,
        scratch_shapes=[
            vmem(w_gate.shape, BF16),
            vmem(w_up.shape, BF16),
            vmem(w_down.shape, BF16),
            vmem(flat, BF16),
            vmem(flat, BF16),
            vmem((n_attn, rows, feat), BF16),
            vmem((n_attn, rows, width), BF16),
            vmem((n_attn, rows, width), F32),
            vmem((width, n_attn * rows), F32),
            vmem((local, pairs, half, slots, 2 * ffn), BF16),
            vmem((local, half, slots, 2 * ffn), BF16),
            vmem((local, half - 1, slots, 2 * ffn), BF16),
            vmem((local, pairs, half, slots, ffn), BF16),
            vmem((n_attn, rows, feat_out), F32),
            vmem((n_attn, rows, feat_out), BF16),
            vmem((n_attn - 1, rows, feat_out), BF16),
            dma((3, local)),
            dma((2,)),
            dma((n_attn - 1,)),
            dma((n_attn - 1,)),
            dma((n_attn - 1,)),
            dma((n_attn - 1,)),
            dma((local,)),
            dma((local,)),
            dma((local, half - 1)),
            dma((local, half - 1)),
            dma((local, half - 1)),
            dma((local, half - 1)),
            dma((local,)),
            dma((local,)),
            dma((n_attn - 1,)),
            dma((n_attn - 1,)),
        ],
        compiler_params=pltpu.CompilerParams(
            collective_id=0, has_side_effects=True, vmem_limit_bytes=52 * 1024 * 1024
        ),
    )(
        tokens, meta, w_gate, w_up, w_down, lengths, query,
        cache_k.reshape(flat), cache_v.reshape(flat),
    )


def body(tokens, expert_ids, gate_weight, w_gate, w_up, w_down, query, cache_k, cache_v, lengths):
    n_attn = lax.axis_size("attn")
    n_exp = lax.axis_size("expert")
    moe_out, attended = routed(
        tokens, expert_ids, gate_weight, w_gate, w_up, w_down,
        query, cache_k, cache_v, lengths, n_attn, n_exp,
    )
    attn_out = attended.reshape(query.shape[0], -1)
    return (moe_out, attn_out)


def solution(mesh):
    return jax.shard_map(
        body,
        mesh=mesh,
        in_specs=(
            P(("groups", "attn"), "expert"),
            P(("groups", "attn"), None),
            P(("groups", "attn"), None),
            P("attn", "expert", None),
            P("attn", "expert", None),
            P("attn", None, "expert"),
            P(("groups", "attn", "expert"), None, None),
            P(("groups", "attn", "expert"), None, None, None),
            P(("groups", "attn", "expert"), None, None, None),
            P(("groups", "attn", "expert")),
        ),
        out_specs=(P(("groups", "attn"), "expert"), P(("groups", "attn", "expert"), None)),
        check_vma=False,
    )
```

```python
import functools

import jax
import jax.numpy as jnp
from jax import lax
from jax.experimental import pallas as pl
from jax.experimental.pallas import tpu as pltpu
from jax.sharding import PartitionSpec as P

F32 = jnp.float32
BF16 = jnp.bfloat16


def remote(src, dst, send_sem, recv_sem, axis, peer):
    return pltpu.make_async_remote_copy(
        src_ref=src,
        dst_ref=dst,
        send_sem=send_sem,
        recv_sem=recv_sem,
        device_id={axis: peer},
        device_id_type=pl.DeviceIdType.MESH,
    )


def attend(length_ref, query_ref, ck_ref, cv_ref, att_ref, kv_count):
    seqs, heads, size = query_ref.shape
    span = ck_ref.shape[1]
    column = lax.broadcasted_iota(jnp.int32, (heads, span), 1)
    row = lax.broadcasted_iota(jnp.int32, (heads, span), 0)
    own = lax.rem(column, kv_count) == row // (heads // kv_count)
    for s in range(seqs):
        scores = lax.dot_general(
            query_ref[s], ck_ref[s], (((1,), (1,)), ((), ())),
            preferred_element_type=F32,
        ) * size ** (-0.5)
        live = own & (column < length_ref[s] * kv_count)
        masked = jnp.where(live, scores, -jnp.inf)
        peak = jnp.max(masked, axis=1, keepdims=True)
        weighted = jnp.exp(masked - peak)
        prob = (weighted / jnp.sum(weighted, axis=1, keepdims=True)).astype(BF16)
        att_ref[s] = jnp.dot(prob, cv_ref[s], preferred_element_type=F32).astype(BF16)


def moe_kernel(
    n_attn,
    n_exp,
    experts,
    kv_count,
    tok_ref,
    meta_ref,
    wg_hbm,
    wu_hbm,
    wd_hbm,
    length_ref,
    query_ref,
    ck_hbm,
    cv_hbm,
    out_ref,
    att_ref,
    wg,
    wu,
    wd,
    ck,
    cv,
    tok_all,
    meta_all,
    pos_col,
    pos_row,
    part,
    pair_in,
    part_in,
    hid,
    acc,
    ret,
    ret_in,
    w_sem,
    c_sem,
    tok_s,
    tok_r,
    meta_s,
    meta_r,
    pair_s,
    pair_r,
    part_s,
    part_r,
    hid_s,
    hid_r,
    back_s,
    back_r,
    ret_s,
    ret_r,
):
    me = lax.axis_index("attn")
    mine = lax.axis_index("expert")
    local = wg.shape[0]
    rows = tok_ref.shape[0]
    feat = tok_ref.shape[1]
    width = meta_ref.shape[1]
    ffn = wg.shape[2]
    pairs, half, slots = part.shape[1:4]
    side = lax.rem(mine, pairs)
    place_in_half = mine // pairs
    capacity = n_exp * slots
    all_rows = n_attn * rows

    def weight_copy(i, j):
        src, dst = ((wg_hbm, wg), (wu_hbm, wu), (wd_hbm, wd))[i]
        return pltpu.make_async_copy(src.at[j], dst.at[j], w_sem.at[i, j])

    for j in range(local):
        weight_copy(0, j).start()
        weight_copy(1, j).start()
    for j in range(local):
        weight_copy(2, j).start()

    ck_copy = pltpu.make_async_copy(ck_hbm, ck, c_sem.at[0])
    cv_copy = pltpu.make_async_copy(cv_hbm, cv, c_sem.at[1])
    ck_copy.start()
    cv_copy.start()

    barrier = pltpu.get_barrier_semaphore()
    for d in range(1, n_attn):
        pl.semaphore_signal(
            barrier, inc=1, device_id={"attn": lax.rem(me + d, n_attn)},
            device_id_type=pl.DeviceIdType.MESH,
        )
    for d in range(1, n_exp):
        pl.semaphore_signal(
            barrier, inc=1, device_id={"expert": lax.rem(mine + d, n_exp)},
            device_id_type=pl.DeviceIdType.MESH,
        )
    pl.semaphore_wait(barrier, n_attn + n_exp - 2)

    def meta_copy(d, slot):
        return remote(meta_ref, meta_all.at[slot], meta_s.at[d - 1], meta_r.at[d - 1],
                      "attn", lax.rem(me + d, n_attn))

    chips = n_attn // 2
    twin = me + 1 - 2 * lax.rem(me, 2)

    def tok_copy(d, slot):
        return remote(tok_ref, tok_all.at[slot], tok_s.at[d - 1], tok_r.at[d - 1],
                      "attn", lax.rem(me + 2 * d, n_attn))

    def tok_twin(d, owner):
        slot = lax.rem(owner + n_attn - 2 * d, n_attn)
        src = tok_all.at[slot] if d else tok_ref
        return remote(src, tok_all.at[slot], tok_s.at[chips - 1 + d],
                      tok_r.at[chips - 1 + d], "attn", twin)

    for d in range(1, n_attn):
        meta_copy(d, me).start()
    for d in range(1, chips):
        tok_copy(d, me).start()
    tok_twin(0, me).start()
    tok_all[me] = tok_ref[...]
    meta_all[me] = meta_ref[...]
    for d in range(1, n_attn):
        meta_copy(d, lax.rem(me + n_attn - d, n_attn)).wait_recv()

    below = (
        lax.broadcasted_iota(jnp.int32, (rows, rows), 0)
        > lax.broadcasted_iota(jnp.int32, (rows, rows), 1)
    ).astype(F32).astype(BF16)
    offset = jnp.zeros((1, width), F32)
    for b in range(n_attn):
        block = meta_all[b]
        place = jnp.dot(below, block, preferred_element_type=F32) + offset
        wide = block.astype(F32)
        offset = offset + jnp.sum(wide, axis=0, keepdims=True)
        place = jnp.where(wide > 0.5, place, -1.0)
        pos_col[b] = place
        pos_row[:, b * rows:(b + 1) * rows] = place.T

    for d in range(1, chips):
        tok_copy(d, lax.rem(me + n_attn - 2 * d, n_attn)).wait_recv()
        tok_twin(d, me).start()
    for d in range(chips):
        tok_twin(d, twin).wait_recv()

    def pair_copy(j):
        return remote(part.at[j, 1 - side], pair_in.at[j], pair_s.at[j], pair_r.at[j],
                      "expert", mine + 1 - 2 * side)

    def part_copy(j, d):
        other = lax.rem(place_in_half + d, half)
        return remote(part.at[j, side, other], part_in.at[j, d - 1], part_s.at[j, d - 1],
                      part_r.at[j, d - 1], "expert", other * pairs + side)

    def hid_copy(j, d, slot):
        other = lax.rem(place_in_half + d, half)
        return remote(hid.at[j, side, place_in_half], hid.at[j, side, slot],
                      hid_s.at[j, d - 1], hid_r.at[j, d - 1], "expert",
                      other * pairs + side)

    def hid_arrive(j):
        for d in range(1, half):
            hid_copy(j, d, lax.rem(place_in_half + half - d, half)).wait_recv()

    def back_copy(j, which):
        return remote(hid.at[j, side], hid.at[j, which], back_s.at[j], back_r.at[j],
                      "expert", mine + 1 - 2 * side)

    def first(j):
        place = pos_row[pl.ds(me * local + j, 1), :].astype(jnp.int32)
        chosen = lax.broadcasted_iota(jnp.int32, (capacity, all_rows), 0) == place
        packed = jnp.dot(
            chosen.astype(F32).astype(BF16),
            tok_all[...].reshape(all_rows, feat),
            preferred_element_type=F32,
        ).astype(BF16)
        weight_copy(0, j).wait()
        weight_copy(1, j).wait()
        gate = jnp.dot(packed, wg[j], preferred_element_type=F32).astype(BF16)
        part[j, :, :, :, :ffn] = gate.reshape(pairs, half, slots, ffn)
        up = jnp.dot(packed, wu[j], preferred_element_type=F32).astype(BF16)
        part[j, :, :, :, ffn:] = up.reshape(pairs, half, slots, ffn)
        if pairs > 1:
            pair_copy(j).start()

    def reduce_pair(j):
        if pairs > 1:
            pair_copy(j).wait_recv()
            part[j, side] = (part[j, side].astype(F32) + pair_in[j].astype(F32)).astype(BF16)
        for d in range(1, half):
            part_copy(j, d).start()

    def second(j):
        for d in range(1, half):
            part_copy(j, d).wait_recv()
        both = part[j, side, place_in_half].astype(F32)
        for d in range(1, half):
            both = both + part_in[j, d - 1].astype(F32)
        gate = both[:, :ffn]
        hid[j, side, place_in_half] = (
            gate / (1.0 + jnp.exp(-gate)) * both[:, ffn:]
        ).astype(BF16)
        for d in range(1, half):
            hid_copy(j, d, place_in_half).start()

    def pass_on(j):
        hid_arrive(j)
        if pairs > 1:
            back_copy(j, side).start()

    acc[...] = jnp.zeros_like(acc)

    def third(j):
        if pairs > 1:
            back_copy(j, 1 - side).wait_recv()
        weight_copy(2, j).wait()
        result = jnp.dot(
            hid[j].reshape(capacity, ffn), wd[j], preferred_element_type=F32
        ).astype(BF16)
        column = me * local + j
        lanes = lax.broadcasted_iota(jnp.int32, (rows, width), 1)
        slot_ids = lax.broadcasted_iota(jnp.int32, (rows, capacity), 1)

        def combine(b, inner):
            place = jnp.sum(
                jnp.where(lanes == column, pos_col[b], 0.0), axis=1, keepdims=True
            ).astype(jnp.int32)
            factor = jnp.sum(
                jnp.where(lanes == column + experts, meta_all[b].astype(F32), 0.0),
                axis=1, keepdims=True,
            )
            spread = jnp.where(slot_ids == place, factor, 0.0).astype(BF16)
            acc[b] = acc[b] + jnp.dot(spread, result, preferred_element_type=F32)
            return inner

        for b in range(n_attn):
            combine(b, 0)

    def step(s, carry):
        for lag, stage in enumerate((first, reduce_pair, second, pass_on, third)):
            if lag == 2:
                @pl.when(s == 1)
                def _():
                    attend(length_ref, query_ref, ck, cv, att_ref, kv_count)

            @pl.when((s >= lag) & (s < local + lag))
            def _():
                stage(s - lag)
        return carry

    ck_copy.wait()
    cv_copy.wait()
    lax.fori_loop(0, local + 4, step, 0)

    ret[...] = acc[...].astype(BF16)

    def ret_copy(d):
        peer = lax.rem(me + d, n_attn)
        return remote(ret.at[peer], ret_in.at[d - 1], ret_s.at[d - 1], ret_r.at[d - 1],
                      "attn", peer)

    for d in range(1, n_attn):
        ret_copy(d).start()
    total = acc[me]
    for d in range(1, n_attn):
        ret_copy(d).wait_recv()
        total = total + ret_in[d - 1].astype(F32)
    out_ref[...] = total.astype(BF16)

    for d in range(1, n_attn):
        meta_copy(d, me).wait_send()
        ret_copy(d).wait_send()

    for d in range(1, chips):
        tok_copy(d, me).wait_send()
    for d in range(chips):
        tok_twin(d, me).wait_send()

    def drain(j, carry):
        if pairs > 1:
            pair_copy(j).wait_send()
            back_copy(j, side).wait_send()
        for d in range(1, half):
            part_copy(j, d).wait_send()
            hid_copy(j, d, place_in_half).wait_send()
        return carry

    lax.fori_loop(0, local, drain, 0)


def routed(tokens, expert_ids, gate_weight, w_gate, w_up, w_down, query, cache_k, cache_v, lengths, n_attn, n_exp):
    rows, feat = tokens.shape
    local, _, ffn = w_gate.shape
    feat_out = w_down.shape[2]
    experts = local * n_attn
    capacity = rows * expert_ids.shape[1] // local
    slots = capacity // n_exp
    pairs = 2 if n_exp > 2 and n_exp % 2 == 0 else 1
    half = n_exp // pairs
    width = -(-2 * experts // 128) * 128
    wanted = jnp.arange(width, dtype=jnp.int32)[None, None, :]
    ids = expert_ids[:, :, None]
    gates = gate_weight.astype(F32)[:, :, None]
    meta = jnp.sum(
        jnp.where(ids == wanted, 1.0, jnp.where(ids + experts == wanted, gates, 0.0)),
        axis=1,
    ).astype(BF16)
    seqs, heads, size = query.shape
    context, kv_count = cache_k.shape[1:3]
    flat = (seqs, context * kv_count, size)
    dma = pltpu.SemaphoreType.DMA
    vmem = pltpu.VMEM
    return pl.pallas_call(
        functools.partial(moe_kernel, n_attn, n_exp, experts, kv_count),
        out_shape=(
            jax.ShapeDtypeStruct((rows, feat_out), BF16),
            jax.ShapeDtypeStruct(query.shape, BF16),
        ),
        in_specs=[pl.BlockSpec(memory_space=pltpu.VMEM)] * 2
        + [pl.BlockSpec(memory_space=pl.ANY)] * 3
        + [pl.BlockSpec(memory_space=pltpu.SMEM)]
        + [pl.BlockSpec(memory_space=pltpu.VMEM)]
        + [pl.BlockSpec(memory_space=pl.ANY)] * 2,
        out_specs=[pl.BlockSpec(memory_space=pltpu.VMEM)] * 2,
        scratch_shapes=[
            vmem(w_gate.shape, BF16),
            vmem(w_up.shape, BF16),
            vmem(w_down.shape, BF16),
            vmem(flat, BF16),
            vmem(flat, BF16),
            vmem((n_attn, rows, feat), BF16),
            vmem((n_attn, rows, width), BF16),
            vmem((n_attn, rows, width), F32),
            vmem((width, n_attn * rows), F32),
            vmem((local, pairs, half, slots, 2 * ffn), BF16),
            vmem((local, half, slots, 2 * ffn), BF16),
            vmem((local, half - 1, slots, 2 * ffn), BF16),
            vmem((local, pairs, half, slots, ffn), BF16),
            vmem((n_attn, rows, feat_out), F32),
            vmem((n_attn, rows, feat_out), BF16),
            vmem((n_attn - 1, rows, feat_out), BF16),
            dma((3, local)),
            dma((2,)),
            dma((n_attn - 1,)),
            dma((n_attn - 1,)),
            dma((n_attn - 1,)),
            dma((n_attn - 1,)),
            dma((local,)),
            dma((local,)),
            dma((local, half - 1)),
            dma((local, half - 1)),
            dma((local, half - 1)),
            dma((local, half - 1)),
            dma((local,)),
            dma((local,)),
            dma((n_attn - 1,)),
            dma((n_attn - 1,)),
        ],
        compiler_params=pltpu.CompilerParams(
            collective_id=0, has_side_effects=True, vmem_limit_bytes=52 * 1024 * 1024
        ),
    )(
        tokens, meta, w_gate, w_up, w_down, lengths, query,
        cache_k.reshape(flat), cache_v.reshape(flat),
    )


def body(tokens, expert_ids, gate_weight, w_gate, w_up, w_down, query, cache_k, cache_v, lengths):
    n_attn = lax.axis_size("attn")
    n_exp = lax.axis_size("expert")
    moe_out, attended = routed(
        tokens, expert_ids, gate_weight, w_gate, w_up, w_down,
        query, cache_k, cache_v, lengths, n_attn, n_exp,
    )
    attn_out = attended.reshape(query.shape[0], -1)
    return (moe_out, attn_out)


def solution(mesh):
    return jax.shard_map(
        body,
        mesh=mesh,
        in_specs=(
            P(("groups", "attn"), "expert"),
            P(("groups", "attn"), None),
            P(("groups", "attn"), None),
            P("attn", "expert", None),
            P("attn", "expert", None),
            P("attn", None, "expert"),
            P(("groups", "attn", "expert"), None, None),
            P(("groups", "attn", "expert"), None, None, None),
            P(("groups", "attn", "expert"), None, None, None),
            P(("groups", "attn", "expert")),
        ),
        out_specs=(P(("groups", "attn"), "expert"), P(("groups", "attn", "expert"), None)),
        check_vma=False,
    )
```
